256 devices in a mesh: orb: 64 (over y, z, core), clu: 4 (over x).
Axes of the slice: x: 4, y: 4, z: 8, core: 2. Of those that a mesh axis runs over, the one named last changes fastest.
Arguments:
- integrals: bfloat16 [1024, 1024, 512], P('orb', 'clu'), may hold values from -1.1953125 to 1.1953125
- metric: bfloat16 [1024, 1024], P(None, 'orb'), may hold values from -0.1875 to 0.1875
- occ_energy: float32 [1024], replicated, may hold values from -2 to -0.5
- virt_energy: float32 [512], replicated, may hold values from 0.5 to 4
- orbital_order: int32 [4, 256], replicated, may hold values from 0 to 255, each once within a row
- pair_first: int32 [4, 64, 4], P('clu', 'orb'), may hold values from 0 to 3
- pair_second: int32 [4, 64, 4], replicated, may hold values from 0 to 255
- pair_live: int32 [4, 64, 4], P('clu', 'orb'), may hold values 0 or 1
Outputs:
- gamma: bfloat16 [1024, 1024, 512], P('orb', 'clu')
The draws below stay inside these ranges and needn't reach their ends.
Inputs may be any that keep to these rules, and one draw needn't show every extreme that they name: `orbital_order`: each row is a permutation of 0 to 255. `pair_second`: slot s names an orbital of cluster s.
All inputs are finite; a program needn't handle non-finite values. No bound on the sum of `pair_live` on one device may be relied on, other than what follows from the above.
Results may differ from the reference program's by a relative error of at most 0.0052.
Values may be sent and summed in bfloat16 or wider, within the bound.
No kernel may reach another device: no remote copies, remote signals or barrier semaphores. Data moves between devices by JAX's collectives and lax.ppermute only.
A program may use at most 128 MiB of HBM per device.

```python
import math
import jax
import jax.numpy as jnp
import numpy as np
from jax import lax

X = 1024
OCC = 256
V = 512
PER_CLU = 1
ORBITALS = 1024
OD = 4
PAIRS = 4
N_ORB = 64
N_CLU = 4


def set_ends(result, key, smallest, top_value):
    spot = [jax.random.randint(jax.random.fold_in(key, axis), (), 0, length) for axis, length in enumerate(result.shape)]
    longest = result.shape.index(max(result.shape))
    next_to = spot[:longest] + [(spot[longest] + 1) % result.shape[longest]] + spot[longest + 1:]
    return result.at[tuple(spot)].set(smallest).at[tuple(next_to)].set(top_value)


def block_levels(own_key, extent, shards, least, high):
    factor_of = 1.0
    for position, parts in shards:
        steps = jax.random.uniform(jax.random.fold_in(jax.random.fold_in(own_key, 6), position), (parts,), jnp.float32, least / len(shards), high / len(shards))
        factor_of = factor_of * jnp.repeat(jnp.exp(steps), extent[position] // parts).reshape((-1,) + (1,) * (len(extent) - 1 - position))
    return factor_of


def rank_bounds(count, skew):
    portions = [(1 << 20) // math.isqrt(standing ** skew) + 1 for standing in range(1, count + 1)]
    scale = 1 + sum(portions) // (1 << 30)
    return np.cumsum(np.array([max(1, weight // scale) for weight in portions]))


def skewed_ids(stream_key, dims, amount, slope):
    listing = rank_bounds(amount, slope)
    ticket = jax.random.randint(jax.random.fold_in(stream_key, 1), dims, 0, int(listing[amount - 1]))
    grade = jnp.searchsorted(jnp.asarray(listing, jnp.int32), ticket, side="right")
    return jax.random.permutation(jax.random.fold_in(stream_key, 2), amount)[grade].astype(jnp.int32)


def scatter_about(rng, dims, deviation, limit, split=(), held_as=jnp.bfloat16):
    array = jax.random.normal(rng, dims, jnp.float32) * deviation
    if len(split) > 0:
        array = block_levels(rng, dims, split, -0.22, 0.18) * array
    return jnp.clip(array, min=-limit, max=limit).astype(held_as)


def setup_inputs(seed: int = 0) -> dict:
    keys = jax.random.split(jax.random.key(seed), 9)
    integrals = scatter_about(keys[0], (X, ORBITALS, V), 0.2, 1.1953125, ((0, 64), (1, 4)))
    metric = scatter_about(keys[1], (X, X), X ** -0.5, 0.1875, ((1, 64),))
    occ_energy = jnp.clip(jax.random.uniform(keys[2], (ORBITALS,), jnp.float32, -2.0, -0.5), -2.0, -0.5)
    virt_energy = jnp.clip(jax.random.uniform(keys[3], (V,), jnp.float32, 0.5, 4.0), 0.5, 4.0)
    orbital_order = jax.vmap(lambda own: jax.random.permutation(own, OCC))(jax.random.split(keys[4], N_CLU)).reshape((N_CLU, OCC)).astype(jnp.int32)
    pair_first = set_ends(jax.random.randint(keys[5], (N_CLU, N_ORB, PAIRS), 0, OD), jax.random.fold_in(keys[5], 1), 0, OD - 1).astype(jnp.int32)
    pair_second = set_ends(skewed_ids(keys[6], (N_CLU, N_ORB, PAIRS), OCC, 2), jax.random.fold_in(keys[6], 3), 0, OCC - 1).astype(jnp.int32)
    pair_live = set_ends((jax.random.randint(keys[7], (N_CLU, N_ORB, PAIRS), 0, 4) < 3).astype(jnp.int32), jax.random.fold_in(keys[7], 1), 0, 1)
    return dict(integrals=integrals, metric=metric, occ_energy=occ_energy, virt_energy=virt_energy, orbital_order=orbital_order, pair_first=pair_first, pair_second=pair_second, pair_live=pair_live)


def reference(integrals, metric, occ_energy, virt_energy, orbital_order, pair_first, pair_second, pair_live):
    owned_count = OCC // N_ORB
    fitted_blocks = []
    for cluster in range(N_CLU):
        cluster_rows = integrals[:, cluster * OCC:(cluster + 1) * OCC, :].reshape(X, OCC * V)
        product = jnp.dot(metric.T, cluster_rows, preferred_element_type=jnp.float32)
        fitted_blocks.append(product.astype(jnp.bfloat16).reshape(X, OCC, V))
    fitted = jnp.concatenate(fitted_blocks, axis=1)
    slot_cluster = (jnp.arange(PAIRS, dtype=jnp.int32) // PER_CLU).astype(jnp.int32)

    def device_gamma(device_index):
        cluster = device_index // N_ORB
        orb_column = device_index % N_ORB
        order_row = orbital_order[cluster]
        owned_orbs = lax.dynamic_slice_in_dim(order_row, orb_column * owned_count, owned_count) + cluster * OCC
        first_slot = pair_first[cluster, orb_column]
        second_orb = pair_second[cluster, orb_column] + slot_cluster * OCC
        live_mask = pair_live[cluster, orb_column].astype(jnp.float32)
        first_orb = jnp.take(owned_orbs, first_slot)
        first_fit = jnp.take(fitted, first_orb, axis=1).astype(jnp.float32)
        second_fit = jnp.take(fitted, second_orb, axis=1).astype(jnp.float32)
        intersection = jnp.einsum("xpa,xpb->pab", first_fit, second_fit)
        denominator = (virt_energy[None, :, None] + virt_energy[None, None, :]
                       - occ_energy[first_orb][:, None, None] - occ_energy[second_orb][:, None, None])
        amplitude = (live_mask[:, None, None] * intersection / denominator).astype(jnp.bfloat16).astype(jnp.float32)
        contribution = jnp.einsum("pab,xpb->xpa", amplitude, second_fit)
        onehot = (first_slot[:, None] == jnp.arange(owned_count, dtype=jnp.int32)[None, :]).astype(jnp.float32)
        gamma_local = jnp.einsum("xpa,pd->xda", contribution, onehot, precision=lax.Precision.HIGHEST)
        return gamma_local.astype(jnp.bfloat16)

    per_device = lax.map(device_gamma, jnp.arange(N_CLU * N_ORB, dtype=jnp.int32))
    per_device = per_device.reshape(N_CLU, N_ORB, X, owned_count, V)
    cluster_gammas = []
    for cluster in range(N_CLU):
        ordered = jnp.transpose(per_device[cluster], (1, 0, 2, 3)).reshape(X, OCC, V)
        inverse = jnp.argsort(orbital_order[cluster]).astype(jnp.int32)
        cluster_gammas.append(jnp.take(ordered, inverse, axis=1))
    return jnp.concatenate(cluster_gammas, axis=1)
```

```python
import functools

import jax
import jax.numpy as jnp
from jax import lax
from jax.experimental import pallas as pl
from jax.experimental.pallas import tpu as pltpu
from jax.sharding import PartitionSpec as P


LANES = 128
NZ, NC = 8, 2


def chosen(clu, rows):
    row = rows[0]
    for i in range(1, len(rows)):
        row = jnp.where(clu == i, rows[i], row)
    return row


def one_hot(row, count):
    lines = lax.broadcasted_iota(jnp.int32, (count, row.shape[1]), 0)
    return (lines == row).astype(jnp.float32)


def pick_kernel(clu_ref, index_ref, raw_ref, out_ref, turned, *, second):
    clu = clu_ref[0]
    xs, occ, width = raw_ref.shape
    if second:
        parts = [
            one_hot(chosen(clu, [index_ref[c, pl.ds(s, 1), :] for s in range(index_ref.shape[1])]), occ).T
            for c in range(index_ref.shape[0])
        ]
        picks = jnp.concatenate(parts, axis=0)
    else:
        picks = one_hot(chosen(clu, [index_ref[pl.ds(c, 1), :] for c in range(index_ref.shape[0])]), occ).T
    picks = picks.astype(jnp.bfloat16)
    count = picks.shape[0]
    for x in range(xs):
        rows = jnp.dot(picks, raw_ref[x], preferred_element_type=jnp.float32)
        for j in range(width // LANES):
            turned[j, pl.ds(x, count, stride=xs), :] = rows[:, j * LANES : (j + 1) * LANES]
    for j in range(width // LANES):
        out_ref[:, j * LANES : (j + 1) * LANES] = turned[j].astype(jnp.bfloat16)


def pick(clu, index, raw, count, second):
    xs, occ, virt = raw.shape
    block = 2 * LANES
    return pl.pallas_call(
        functools.partial(pick_kernel, second=second),
        grid=(virt // block,),
        in_specs=[
            pl.BlockSpec(memory_space=pltpu.SMEM),
            pl.BlockSpec(index.shape, lambda v: (0,) * index.ndim),
            pl.BlockSpec((xs, occ, block), lambda v: (0, 0, v)),
        ],
        out_specs=pl.BlockSpec((count * xs, block), lambda v: (0, v)),
        out_shape=jax.ShapeDtypeStruct((count * xs, virt), jnp.bfloat16),
        scratch_shapes=[pltpu.VMEM((block // LANES, count * xs, LANES), jnp.float32)],
        cost_estimate=pl.CostEstimate(
            flops=2 * xs * count * occ * virt, bytes_accessed=2 * xs * (count + occ) * virt, transcendentals=0
        ),
        name="pick_second" if second else "pick_owned",
    )(clu, index, raw)


def place_kernel(clu_ref, order_ref, back_ref, out_ref, turned):
    clu = clu_ref[0]
    xs, occ, width = out_ref.shape
    spots = one_hot(
        chosen(clu, [order_ref[pl.ds(c, 1), :] for c in range(order_ref.shape[0])]), occ
    ).astype(jnp.bfloat16)
    for j in range(width // LANES):
        turned[j] = back_ref[:, j * LANES : (j + 1) * LANES].astype(jnp.float32)
    for x in range(xs):
        rows = jnp.concatenate(
            [turned[j, pl.ds(x, occ, stride=xs), :] for j in range(width // LANES)], axis=1
        ).astype(jnp.bfloat16)
        out_ref[x] = jnp.dot(spots, rows, preferred_element_type=jnp.float32).astype(jnp.bfloat16)


def place(clu, order, back, xs):
    occ = order.shape[1]
    virt = back.shape[1]
    block = 2 * LANES
    return pl.pallas_call(
        place_kernel,
        grid=(virt // block,),
        in_specs=[
            pl.BlockSpec(memory_space=pltpu.SMEM),
            pl.BlockSpec(order.shape, lambda v: (0, 0)),
            pl.BlockSpec((occ * xs, block), lambda v: (0, v)),
        ],
        out_specs=pl.BlockSpec((xs, occ, block), lambda v: (0, 0, v)),
        out_shape=jax.ShapeDtypeStruct((xs, occ, virt), jnp.bfloat16),
        scratch_shapes=[pltpu.VMEM((block // LANES, occ * xs, LANES), jnp.float32)],
        cost_estimate=pl.CostEstimate(
            flops=2 * xs * occ * occ * virt, bytes_accessed=4 * xs * occ * virt, transcendentals=0
        ),
        name="place",
    )(clu, order, back)


def gamma_kernel(
    first_ref, scale_ref, own_ref, weight_ref, fit_ref, virt_row_ref, virt_col_ref, out_ref, total
):
    slot = pl.program_id(0)
    sources, _, xs, virt = own_ref.shape
    first = first_ref[slot]

    @pl.when(slot == 0)
    def _():
        total[...] = jnp.zeros(total.shape, total.dtype)

    raw = own_ref[:, 0].reshape(sources * xs, virt)
    crossed = jnp.dot(weight_ref[0], raw, preferred_element_type=jnp.float32)
    below = virt_col_ref[...] + virt_row_ref[...] - scale_ref[0, slot] - scale_ref[1, slot]
    amplitude = (scale_ref[2, slot] * crossed / below).astype(jnp.bfloat16)
    total[first] += jnp.dot(fit_ref[0], amplitude, preferred_element_type=jnp.float32)

    @pl.when(slot == pl.num_programs(0) - 1)
    def _():
        for k in range(out_ref.shape[1]):
            out_ref[:, k] = total[k].astype(jnp.bfloat16).reshape(sources, xs, virt)


def gamma_of(first, scale, own, weight, fit, virt_energy):
    sources, owned, xs, virt = own.shape
    slots, _, full = weight.shape
    return pl.pallas_call(
        gamma_kernel,
        grid_spec=pltpu.PrefetchScalarGridSpec(
            num_scalar_prefetch=2,
            grid=(slots,),
            in_specs=[
                pl.BlockSpec((sources, 1, xs, virt), lambda s, first, scale: (0, first[s], 0, 0)),
                pl.BlockSpec((1, virt, full), lambda s, first, scale: (s, 0, 0)),
                pl.BlockSpec((1, full, virt), lambda s, first, scale: (s, 0, 0)),
                pl.BlockSpec((1, virt), lambda s, first, scale: (0, 0)),
                pl.BlockSpec((virt, 1), lambda s, first, scale: (0, 0)),
            ],
            out_specs=pl.BlockSpec((sources, owned, xs, virt), lambda s, first, scale: (0, 0, 0, 0)),
            scratch_shapes=[pltpu.VMEM((owned, full, virt), jnp.float32)],
        ),
        out_shape=jax.ShapeDtypeStruct(own.shape, jnp.bfloat16),
        cost_estimate=pl.CostEstimate(
            flops=4 * slots * full * virt * virt, bytes_accessed=16 * full * virt * 2, transcendentals=0
        ),
        compiler_params=pltpu.CompilerParams(vmem_limit_bytes=48 * 1024 * 1024),
        name="gamma",
    )(first, scale, own, weight, fit, virt_energy[None, :], virt_energy[:, None])


def ring_gather(block, here, count, step):
    got = [block] + [lax.ppermute(block, "orb", step(k)) for k in range(1, count)]
    return jnp.take(jnp.stack(got), (here - jnp.arange(count)) % count, axis=0, mode="clip")


def whole_metric(metric):
    orb_count = lax.axis_size("orb")
    ny = orb_count // (NZ * NC)
    here = lax.axis_index("orb")
    spots = [(y, z, c) for y in range(ny) for z in range(NZ) for c in range(NC)]
    number = lambda y, z, c: (y * NZ + z) * NC + c
    along_z = lambda k: [(number(y, z, c), number(y, (z + k) % NZ, c)) for y, z, c in spots]

    def across(k):
        pairs = []
        for y, z, c in spots:
            g = (y * NC + c + k) % (ny * NC)
            pairs.append((number(y, z, c), number(g // NC, z, g % NC)))
        return pairs

    here_z = (here // NC) % NZ
    here_g = (here // (NZ * NC)) * NC + here % NC
    mine = metric.T
    column = ring_gather(mine, here_z, NZ, along_z)
    parts = ring_gather(column, here_g, ny * NC, across)
    q, p = mine.shape
    parts = parts.reshape(ny, NC, NZ, q, p).transpose(0, 2, 1, 3, 4)
    return parts.reshape(orb_count * q, p)


def on_device(
    integrals, metric, occ_energy, virt_energy, orbital_order, pair_first, pair_second, pair_live
):
    orb_count = lax.axis_size("orb")
    here_orb = lax.axis_index("orb")
    here_clu = lax.axis_index("clu")
    xs_rows, occ_count, virt = integrals.shape
    full_aux = metric.shape[0]
    owned = occ_count // orb_count
    slots = pair_second.shape[2]
    clu = here_clu.astype(jnp.int32)[None]

    wanted = pick(clu, pair_second.transpose(0, 2, 1), integrals, occ_count, True)
    seconds = lax.all_to_all(
        wanted.reshape(-1, xs_rows, virt), ("clu", "orb"), split_axis=0, concat_axis=0, tiled=True
    ).reshape(slots, full_aux, virt)

    mine = pick(clu, orbital_order, integrals, occ_count, False)
    own = lax.all_to_all(
        mine.reshape(orb_count, owned, xs_rows, virt), "orb", split_axis=0, concat_axis=0, tiled=True
    )

    turned = whole_metric(metric)
    fit = jnp.einsum("qp,spb->sqb", turned, seconds, preferred_element_type=jnp.float32).astype(jnp.bfloat16)
    weight = jnp.einsum("sqb,qp->sbp", fit, turned, preferred_element_type=jnp.float32).astype(jnp.bfloat16)

    first_slot = pair_first[0, 0]
    order = lax.dynamic_index_in_dim(orbital_order, here_clu, 0, keepdims=False)
    owned_orbs = lax.dynamic_slice_in_dim(order, here_orb * owned, owned) + here_clu * occ_count
    first_orb = jnp.take(owned_orbs, first_slot)
    own_second = lax.dynamic_slice(pair_second, (here_clu, here_orb, 0), (1, 1, slots))[0, 0]
    second_orb = own_second + jnp.arange(slots, dtype=jnp.int32) * occ_count
    scale = jnp.stack(
        [occ_energy[first_orb], occ_energy[second_orb], pair_live[0, 0].astype(jnp.float32)]
    )

    local = gamma_of(first_slot, scale, own, weight, fit, virt_energy)
    back = lax.all_to_all(local, "orb", split_axis=0, concat_axis=0, tiled=True)
    return place(clu, orbital_order, back.reshape(occ_count * xs_rows, virt), xs_rows)


def solution(mesh):
    in_specs = (
        P("orb", "clu", None),
        P(None, "orb"),
        P(),
        P(),
        P(),
        P("clu", "orb", None),
        P(),
        P("clu", "orb", None),
    )
    out_specs = P("orb", "clu", None)
    return jax.shard_map(
        on_device, mesh=mesh, in_specs=in_specs, out_specs=out_specs, check_vma=False
    )
```

```python
import functools

import jax
import jax.numpy as jnp
from jax import lax
from jax.experimental import pallas as pl
from jax.experimental.pallas import tpu as pltpu
from jax.sharding import PartitionSpec as P


LANES = 128
NZ, NC = 8, 2


def chosen(clu, rows):
    row = rows[0]
    for i in range(1, len(rows)):
        row = jnp.where(clu == i, rows[i], row)
    return row


def one_hot(row, count):
    lines = lax.broadcasted_iota(jnp.int32, (count, row.shape[1]), 0)
    return (lines == row).astype(jnp.float32)


def pick_kernel(clu_ref, index_ref, raw_ref, out_ref, turned, *, second):
    clu = clu_ref[0]
    xs, occ, width = raw_ref.shape
    if second:
        parts = [
            one_hot(chosen(clu, [index_ref[c, pl.ds(s, 1), :] for s in range(index_ref.shape[1])]), occ).T
            for c in range(index_ref.shape[0])
        ]
        picks = jnp.concatenate(parts, axis=0)
    else:
        picks = one_hot(chosen(clu, [index_ref[pl.ds(c, 1), :] for c in range(index_ref.shape[0])]), occ).T
    picks = picks.astype(jnp.bfloat16)
    count = picks.shape[0]
    for x in range(xs):
        rows = jnp.dot(picks, raw_ref[x], preferred_element_type=jnp.float32)
        for j in range(width // LANES):
            turned[j, pl.ds(x, count, stride=xs), :] = rows[:, j * LANES : (j + 1) * LANES]
    for j in range(width // LANES):
        out_ref[:, j * LANES : (j + 1) * LANES] = turned[j].astype(jnp.bfloat16)


def pick(clu, index, raw, count, second):
    xs, occ, virt = raw.shape
    block = 2 * LANES
    return pl.pallas_call(
        functools.partial(pick_kernel, second=second),
        grid=(virt // block,),
        in_specs=[
            pl.BlockSpec(memory_space=pltpu.SMEM),
            pl.BlockSpec(index.shape, lambda v: (0,) * index.ndim),
            pl.BlockSpec((xs, occ, block), lambda v: (0, 0, v)),
        ],
        out_specs=pl.BlockSpec((count * xs, block), lambda v: (0, v)),
        out_shape=jax.ShapeDtypeStruct((count * xs, virt), jnp.bfloat16),
        scratch_shapes=[pltpu.VMEM((block // LANES, count * xs, LANES), jnp.float32)],
        cost_estimate=pl.CostEstimate(
            flops=2 * xs * count * occ * virt, bytes_accessed=2 * xs * (count + occ) * virt, transcendentals=0
        ),
        name="pick_second" if second else "pick_owned",
    )(clu, index, raw)


def place_kernel(clu_ref, order_ref, back_ref, out_ref, turned):
    clu = clu_ref[0]
    xs, occ, width = out_ref.shape
    spots = one_hot(
        chosen(clu, [order_ref[pl.ds(c, 1), :] for c in range(order_ref.shape[0])]), occ
    ).astype(jnp.bfloat16)
    for j in range(width // LANES):
        turned[j] = back_ref[:, j * LANES : (j + 1) * LANES].astype(jnp.float32)
    for x in range(xs):
        rows = jnp.concatenate(
            [turned[j, pl.ds(x, occ, stride=xs), :] for j in range(width // LANES)], axis=1
        ).astype(jnp.bfloat16)
        out_ref[x] = jnp.dot(spots, rows, preferred_element_type=jnp.float32).astype(jnp.bfloat16)


def place(clu, order, back, xs):
    occ = order.shape[1]
    virt = back.shape[1]
    block = 2 * LANES
    return pl.pallas_call(
        place_kernel,
        grid=(virt // block,),
        in_specs=[
            pl.BlockSpec(memory_space=pltpu.SMEM),
            pl.BlockSpec(order.shape, lambda v: (0, 0)),
            pl.BlockSpec((occ * xs, block), lambda v: (0, v)),
        ],
        out_specs=pl.BlockSpec((xs, occ, block), lambda v: (0, 0, v)),
        out_shape=jax.ShapeDtypeStruct((xs, occ, virt), jnp.bfloat16),
        scratch_shapes=[pltpu.VMEM((block // LANES, occ * xs, LANES), jnp.float32)],
        cost_estimate=pl.CostEstimate(
            flops=2 * xs * occ * occ * virt, bytes_accessed=4 * xs * occ * virt, transcendentals=0
        ),
        name="place",
    )(clu, order, back)


def gamma_kernel(
    first_ref, scale_ref, own_ref, weight_ref, fit_ref, virt_row_ref, virt_col_ref, out_ref, total
):
    slot = pl.program_id(0)
    sources, _, xs, virt = own_ref.shape
    first = first_ref[slot]

    @pl.when(slot == 0)
    def _():
        total[...] = jnp.zeros(total.shape, total.dtype)

    raw = own_ref[:, 0].reshape(sources * xs, virt)
    crossed = jnp.dot(weight_ref[0], raw, preferred_element_type=jnp.float32)
    below = virt_col_ref[...] + virt_row_ref[...] - scale_ref[0, slot] - scale_ref[1, slot]
    amplitude = (scale_ref[2, slot] * crossed / below).astype(jnp.bfloat16)
    total[first] += jnp.dot(fit_ref[0], amplitude, preferred_element_type=jnp.float32)

    @pl.when(slot == pl.num_programs(0) - 1)
    def _():
        for k in range(out_ref.shape[1]):
            out_ref[:, k] = total[k].astype(jnp.bfloat16).reshape(sources, xs, virt)


def gamma_of(first, scale, own, weight, fit, virt_energy):
    sources, owned, xs, virt = own.shape
    slots, _, full = weight.shape
    return pl.pallas_call(
        gamma_kernel,
        grid_spec=pltpu.PrefetchScalarGridSpec(
            num_scalar_prefetch=2,
            grid=(slots,),
            in_specs=[
                pl.BlockSpec((sources, 1, xs, virt), lambda s, first, scale: (0, first[s], 0, 0)),
                pl.BlockSpec((1, virt, full), lambda s, first, scale: (s, 0, 0)),
                pl.BlockSpec((1, full, virt), lambda s, first, scale: (s, 0, 0)),
                pl.BlockSpec((1, virt), lambda s, first, scale: (0, 0)),
                pl.BlockSpec((virt, 1), lambda s, first, scale: (0, 0)),
            ],
            out_specs=pl.BlockSpec((sources, owned, xs, virt), lambda s, first, scale: (0, 0, 0, 0)),
            scratch_shapes=[pltpu.VMEM((owned, full, virt), jnp.float32)],
        ),
        out_shape=jax.ShapeDtypeStruct(own.shape, jnp.bfloat16),
        cost_estimate=pl.CostEstimate(
            flops=4 * slots * full * virt * virt, bytes_accessed=16 * full * virt * 2, transcendentals=0
        ),
        compiler_params=pltpu.CompilerParams(vmem_limit_bytes=48 * 1024 * 1024),
        name="gamma",
    )(first, scale, own, weight, fit, virt_energy[None, :], virt_energy[:, None])


def whole_metric(metric):
    orb_count = lax.axis_size("orb")
    ny = orb_count // (NZ * NC)
    half = NZ // 2
    here = lax.axis_index("orb")
    here_y, here_h, here_l, here_c = here // (NZ * NC), here // (2 * NC) % half, here // NC % 2, here % NC

    def send(block, to):
        pairs = []
        for y in range(ny):
            for h in range(half):
                for l in range(2):
                    for c in range(NC):
                        y2, h2, l2, c2 = to(y, h, l, c)
                        pairs.append(
                            (((y * half + h) * 2 + l) * NC + c, ((y2 * half + h2) * 2 + l2) * NC + c2)
                        )
        return lax.ppermute(block, "orb", pairs)

    def both(mine, other, here):
        return jnp.stack([jnp.where(here == 0, mine, other), jnp.where(here == 0, other, mine)])

    block = metric.T
    q, p = block.shape
    got = [send(block, lambda y, h, l, c, r=r: (y, (h + r) % half, l, c)) for r in range(1, half)]
    column = jnp.stack([block] + got)
    other = send(column, lambda y, h, l, c: (y, h, 1 - l, c))
    column = both(column, other, here_l)
    got = [send(column, lambda y, h, l, c, t=t: ((y + t) % ny, h, l, c)) for t in range(1, ny)]
    plane = jnp.stack([column] + got)
    other = send(plane, lambda y, h, l, c: (y, h, l, 1 - c))
    every = jnp.stack([plane, other]).reshape(orb_count, q, p)
    place = jnp.arange(orb_count, dtype=jnp.int32)
    y, h, l, c = place // (NZ * NC), place // (2 * NC) % half, place // NC % 2, place % NC
    spot = (((c + here_c) % NC * ny + (here_y - y) % ny) * 2 + l) * half + (here_h - h) % half
    return jnp.take(every, spot, axis=0, mode="clip").reshape(orb_count * q, p)


def window(
    integrals, metric, occ_energy, virt_energy, orbital_order, pair_first, pair_second, pair_live
):
    orb_count = lax.axis_size("orb")
    here_orb = lax.axis_index("orb")
    here_clu = lax.axis_index("clu")
    xs_rows, occ_count, virt = integrals.shape
    full_aux = metric.shape[0]
    owned = occ_count // orb_count
    slots = pair_second.shape[2]
    clu = here_clu.astype(jnp.int32)[None]

    wanted = pick(clu, pair_second.transpose(0, 2, 1), integrals, occ_count, True)
    seconds = lax.all_to_all(
        wanted.reshape(-1, xs_rows, virt), ("clu", "orb"), split_axis=0, concat_axis=0, tiled=True
    ).reshape(slots, full_aux, virt)

    mine = pick(clu, orbital_order, integrals, occ_count, False)
    own = lax.all_to_all(mine.reshape(orb_count, owned, xs_rows, virt), "orb", split_axis=0, concat_axis=0, tiled=True)

    turned = whole_metric(metric)
    fit = jnp.einsum("qp,spb->sqb", turned, seconds, preferred_element_type=jnp.float32).astype(jnp.bfloat16)
    weight = jnp.einsum("sqb,qp->sbp", fit, turned, preferred_element_type=jnp.float32).astype(jnp.bfloat16)

    first_slot = pair_first[0, 0]
    order = lax.dynamic_index_in_dim(orbital_order, here_clu, 0, keepdims=False)
    owned_orbs = lax.dynamic_slice_in_dim(order, here_orb * owned, owned) + here_clu * occ_count
    first_orb = jnp.take(owned_orbs, first_slot)
    own_second = lax.dynamic_slice(pair_second, (here_clu, here_orb, 0), (1, 1, slots))[0, 0]
    second_orb = own_second + jnp.arange(slots, dtype=jnp.int32) * occ_count
    scale = jnp.stack(
        [occ_energy[first_orb], occ_energy[second_orb], pair_live[0, 0].astype(jnp.float32)]
    )

    local = gamma_of(first_slot, scale, own, weight, fit, virt_energy)
    back = lax.all_to_all(local, "orb", split_axis=0, concat_axis=0, tiled=True)
    return place(clu, orbital_order, back.reshape(occ_count * xs_rows, virt), xs_rows)


def solution(mesh):
    in_specs = (
        P("orb", "clu", None),
        P(None, "orb"),
        P(),
        P(),
        P(),
        P("clu", "orb", None),
        P(),
        P("clu", "orb", None),
    )
    out_specs = P("orb", "clu", None)
    return jax.shard_map(window, mesh=mesh, in_specs=in_specs, out_specs=out_specs, check_vma=False)
```

```python
import functools

import jax
import jax.numpy as jnp
from jax import lax
from jax.experimental import pallas as pl
from jax.experimental.pallas import tpu as pltpu
from jax.sharding import PartitionSpec as P


BLOCK, GROUP = 256, 16
NZ, NC = 8, 2


def chosen(clu, rows):
    row = rows[0]
    for i in range(1, len(rows)):
        row = jnp.where(clu == i, rows[i], row)
    return row


def one_hot(row, count):
    lines = lax.broadcasted_iota(jnp.int32, (count, row.shape[1]), 0)
    return (lines == row).astype(jnp.float32)


def turning(rows, cols):
    count = rows * cols
    to = lax.broadcasted_iota(jnp.int32, (count, count), 0)
    at = lax.broadcasted_iota(jnp.int32, (count, count), 1)
    return ((at // cols == to % rows) & (at % cols == to // rows)).astype(jnp.float32).astype(jnp.bfloat16)


def pick_kernel(clu_ref, index_ref, raw_ref, out_ref, middle, *, second):
    clu = clu_ref[0]
    xs, occ, width = raw_ref.shape
    if second:
        parts = [
            one_hot(chosen(clu, [index_ref[c, pl.ds(s, 1), :] for s in range(index_ref.shape[1])]), occ).T
            for c in range(index_ref.shape[0])
        ]
        picks = jnp.concatenate(parts, axis=0)
    else:
        picks = one_hot(chosen(clu, [index_ref[pl.ds(c, 1), :] for c in range(index_ref.shape[0])]), occ).T
    picks = picks.astype(jnp.bfloat16)
    for x in range(xs):
        middle[x] = jnp.dot(picks, raw_ref[x], preferred_element_type=jnp.float32).astype(jnp.bfloat16)
    turn = turning(xs, GROUP)
    for g in range(picks.shape[0] // GROUP):
        lines = middle[:, g * GROUP : (g + 1) * GROUP, :].reshape(xs * GROUP, width)
        out_ref[g * GROUP * xs : (g + 1) * GROUP * xs, :] = jnp.dot(
            turn, lines, preferred_element_type=jnp.float32
        ).astype(jnp.bfloat16)


def pick(clu, index, raw, count, second):
    xs, occ, virt = raw.shape
    return pl.pallas_call(
        functools.partial(pick_kernel, second=second),
        grid=(virt // BLOCK,),
        in_specs=[
            pl.BlockSpec(memory_space=pltpu.SMEM),
            pl.BlockSpec(index.shape, lambda v: (0,) * index.ndim),
            pl.BlockSpec((xs, occ, BLOCK), lambda v: (0, 0, v)),
        ],
        out_specs=pl.BlockSpec((count * xs, BLOCK), lambda v: (0, v)),
        out_shape=jax.ShapeDtypeStruct((count * xs, virt), jnp.bfloat16),
        scratch_shapes=[pltpu.VMEM((xs, count, BLOCK), jnp.bfloat16)],
        cost_estimate=pl.CostEstimate(
            flops=4 * xs * count * occ * virt, bytes_accessed=2 * xs * (count + occ) * virt, transcendentals=0
        ),
        name="pick_second" if second else "pick_owned",
    )(clu, index, raw)


def place_kernel(clu_ref, order_ref, back_ref, out_ref, middle):
    clu = clu_ref[0]
    xs, occ, width = out_ref.shape
    spots = one_hot(
        chosen(clu, [order_ref[pl.ds(c, 1), :] for c in range(order_ref.shape[0])]), occ
    ).astype(jnp.bfloat16)
    turn = turning(GROUP, xs)
    for g in range(occ // GROUP):
        lines = back_ref[g * GROUP * xs : (g + 1) * GROUP * xs, :]
        middle[:, g * GROUP : (g + 1) * GROUP, :] = (
            jnp.dot(turn, lines, preferred_element_type=jnp.float32)
            .astype(jnp.bfloat16)
            .reshape(xs, GROUP, width)
        )
    for x in range(xs):
        out_ref[x] = jnp.dot(spots, middle[x], preferred_element_type=jnp.float32).astype(jnp.bfloat16)


def place(clu, order, back, xs):
    occ = order.shape[1]
    virt = back.shape[1]
    return pl.pallas_call(
        place_kernel,
        grid=(virt // BLOCK,),
        in_specs=[
            pl.BlockSpec(memory_space=pltpu.SMEM),
            pl.BlockSpec(order.shape, lambda v: (0, 0)),
            pl.BlockSpec((occ * xs, BLOCK), lambda v: (0, v)),
        ],
        out_specs=pl.BlockSpec((xs, occ, BLOCK), lambda v: (0, 0, v)),
        out_shape=jax.ShapeDtypeStruct((xs, occ, virt), jnp.bfloat16),
        scratch_shapes=[pltpu.VMEM((xs, occ, BLOCK), jnp.bfloat16)],
        cost_estimate=pl.CostEstimate(
            flops=4 * xs * occ * occ * virt, bytes_accessed=4 * xs * occ * virt, transcendentals=0
        ),
        name="place",
    )(clu, order, back)


def gamma_kernel(
    slot_ref, first_ref, scale_ref, virt_row_ref, virt_col_ref, own_hbm, weight_hbm, fit_hbm, out_hbm,
    own, weight, fit, amplitude, total, rounded, blank, own_in, weight_in, fit_in, sent, blanked,
):
    slots = weight.shape[0]
    owned = out_hbm.shape[1]
    full, virt = total.shape
    slot = [slot_ref[t] for t in range(slots)]
    first = [first_ref[t] for t in range(slots)]
    used = [functools.reduce(jnp.logical_or, [f == k for f in first]) for k in range(owned)]
    copy = pltpu.make_async_copy
    own_copy = [copy(own_hbm.at[:, first[t]], own.at[t], own_in.at[t]) for t in range(slots)]
    weight_copy = [copy(weight_hbm.at[slot[t]], weight.at[t], weight_in.at[t]) for t in range(slots)]
    fit_copy = [copy(fit_hbm.at[slot[t]], fit.at[t], fit_in.at[t]) for t in range(slots)]
    send = [copy(rounded.at[t], out_hbm.at[:, first[t]], sent.at[t]) for t in range(slots)]
    clear = [copy(blank, out_hbm.at[:, k], blanked.at[k]) for k in range(owned)]
    for t in range(slots):
        own_copy[t].start()
        weight_copy[t].start()
        fit_copy[t].start()
    blank[...] = jnp.zeros(blank.shape, blank.dtype)
    for k in range(owned):
        @pl.when(jnp.logical_not(used[k]))
        def _(k=k):
            clear[k].start()

    for t in range(slots):
        own_copy[t].wait()
        weight_copy[t].wait()
        crossed = jnp.dot(weight[t], own[t].reshape(full, virt), preferred_element_type=jnp.float32)
        below = virt_col_ref[...] + virt_row_ref[...] - scale_ref[0, slot[t]] - scale_ref[1, slot[t]]
        amplitude[...] = (crossed * (scale_ref[2, slot[t]] / below)).astype(jnp.bfloat16)
        fit_copy[t].wait()
        part = jnp.dot(fit[t], amplitude[...], preferred_element_type=jnp.float32)
        if t > 0:
            part = part + jnp.where(first[t] == first[t - 1], total[...], 0.0)
        if t < slots - 1:
            total[...] = part
        rounded[t] = part.astype(jnp.bfloat16).reshape(rounded.shape[1:])
        if t < slots - 1:
            @pl.when(first[t] != first[t + 1])
            def _(t=t):
                send[t].start()
        else:
            send[t].start()

    for t in range(slots - 1):
        @pl.when(first[t] != first[t + 1])
        def _(t=t):
            send[t].wait()

    send[slots - 1].wait()
    for k in range(owned):
        @pl.when(jnp.logical_not(used[k]))
        def _(k=k):
            clear[k].wait()


def gamma_of(first, scale, own, weight, fit, virt_energy):
    sources, owned, xs, virt = own.shape
    slots, _, full = weight.shape
    number = jnp.arange(slots, dtype=jnp.int32)
    key = first * slots + number
    rank = jnp.sum((key[:, None] > key[None, :]).astype(jnp.int32), axis=1)
    at = (rank[None, :] == number[:, None]).astype(jnp.int32)
    hbm = pl.BlockSpec(memory_space=pltpu.HBM)
    smem = pl.BlockSpec(memory_space=pltpu.SMEM)
    vmem = pl.BlockSpec(memory_space=pltpu.VMEM)
    dma = pltpu.SemaphoreType.DMA
    return pl.pallas_call(
        gamma_kernel,
        in_specs=[smem, smem, smem, vmem, vmem, hbm, hbm, hbm],
        out_specs=hbm,
        out_shape=jax.ShapeDtypeStruct(own.shape, jnp.bfloat16),
        scratch_shapes=[
            pltpu.VMEM((slots, sources, xs, virt), jnp.bfloat16),
            pltpu.VMEM((slots, virt, full), jnp.bfloat16),
            pltpu.VMEM((slots, full, virt), jnp.bfloat16),
            pltpu.VMEM((virt, virt), jnp.bfloat16),
            pltpu.VMEM((full, virt), jnp.float32),
            pltpu.VMEM((slots, sources, xs, virt), jnp.bfloat16),
            pltpu.VMEM((sources, xs, virt), jnp.bfloat16),
            dma((slots,)),
            dma((slots,)),
            dma((slots,)),
            dma((slots,)),
            dma((owned,)),
        ],
        cost_estimate=pl.CostEstimate(
            flops=4 * slots * full * virt * virt, bytes_accessed=16 * full * virt * 2, transcendentals=0
        ),
        compiler_params=pltpu.CompilerParams(vmem_limit_bytes=52 * 1024 * 1024),
        name="gamma",
    )(
        jnp.sum(at * number[None, :], axis=1),
        jnp.sum(at * first[None, :], axis=1),
        scale,
        virt_energy[None, :],
        virt_energy[:, None],
        own,
        weight,
        fit,
    )


def whole_metric(metric):
    orb_count = lax.axis_size("orb")
    ny = orb_count // (NZ * NC)
    here = lax.axis_index("orb")
    here_y, here_z, here_c = here // (NZ * NC), here // NC % NZ, here % NC
    spots = [(y, z, c) for y in range(ny) for z in range(NZ) for c in range(NC)]

    def send(block, dy, dz, dc):
        pairs = [
            (
                (y * NZ + z) * NC + c,
                ((y + dy) % ny * NZ + (z + dz) % NZ) * NC + (c + dc) % NC,
            )
            for y, z, c in spots
        ]
        return lax.ppermute(block, "orb", pairs)

    block = metric.T
    q, p = block.shape
    got = [send(block, 0, k, 0) for k in range(1, NZ)]
    column = jnp.stack([block] + got)
    got = [send(column, k, 0, 0) for k in range(1, ny)]
    plane = jnp.stack([column] + got)
    got = [send(plane, 0, 0, k) for k in range(1, NC)]
    every = jnp.stack([plane] + got).reshape(orb_count, q, p)
    place = jnp.arange(orb_count, dtype=jnp.int32)
    y, z, c = place // (NZ * NC), place // NC % NZ, place % NC
    spot = ((here_c - c) % NC * ny + (here_y - y) % ny) * NZ + (here_z - z) % NZ
    return jnp.take(every, spot, axis=0, mode="clip").reshape(orb_count * q, p)


def window(
    integrals, metric, occ_energy, virt_energy, orbital_order, pair_first, pair_second, pair_live
):
    orb_count = lax.axis_size("orb")
    here_orb = lax.axis_index("orb")
    here_clu = lax.axis_index("clu")
    xs_rows, occ_count, virt = integrals.shape
    full_aux = metric.shape[0]
    owned = occ_count // orb_count
    slots = pair_second.shape[2]
    clu = here_clu.astype(jnp.int32)[None]

    wanted = pick(clu, pair_second.transpose(0, 2, 1), integrals, occ_count, True)
    seconds = lax.all_to_all(
        wanted.reshape(-1, xs_rows, virt), ("clu", "orb"), split_axis=0, concat_axis=0, tiled=True
    ).reshape(slots, full_aux, virt)

    mine = pick(clu, orbital_order, integrals, occ_count, False)
    own = lax.all_to_all(mine.reshape(orb_count, owned, xs_rows, virt), "orb", split_axis=0, concat_axis=0, tiled=True)

    turned = whole_metric(metric)
    fit = jnp.einsum("qp,spb->sqb", turned, seconds, preferred_element_type=jnp.float32).astype(jnp.bfloat16)
    weight = jnp.einsum("sqb,qp->sbp", fit, turned, preferred_element_type=jnp.float32).astype(jnp.bfloat16)

    first_slot = pair_first[0, 0]
    order = lax.dynamic_index_in_dim(orbital_order, here_clu, 0, keepdims=False)
    owned_orbs = lax.dynamic_slice_in_dim(order, here_orb * owned, owned) + here_clu * occ_count
    first_orb = jnp.take(owned_orbs, first_slot)
    own_second = lax.dynamic_slice(pair_second, (here_clu, here_orb, 0), (1, 1, slots))[0, 0]
    second_orb = own_second + jnp.arange(slots, dtype=jnp.int32) * occ_count
    scale = jnp.stack(
        [occ_energy[first_orb], occ_energy[second_orb], pair_live[0, 0].astype(jnp.float32)]
    )

    local = gamma_of(first_slot, scale, own, weight, fit, virt_energy)
    back = lax.all_to_all(local, "orb", split_axis=0, concat_axis=0, tiled=True)
    return place(clu, orbital_order, back.reshape(occ_count * xs_rows, virt), xs_rows)


def solution(mesh):
    in_specs = (
        P("orb", "clu", None),
        P(None, "orb"),
        P(),
        P(),
        P(),
        P("clu", "orb", None),
        P(),
        P("clu", "orb", None),
    )
    out_specs = P("orb", "clu", None)
    return jax.shard_map(window, mesh=mesh, in_specs=in_specs, out_specs=out_specs, check_vma=False)
```

```python
import functools

import jax
import jax.numpy as jnp
from jax import lax
from jax.experimental import pallas as pl
from jax.experimental.pallas import tpu as pltpu
from jax.sharding import PartitionSpec as P


BLOCK, GROUP = 256, 16
PARTS = 4
NZ, NC = 8, 2


def chosen(clu, rows):
    row = rows[0]
    for i in range(1, len(rows)):
        row = jnp.where(clu == i, rows[i], row)
    return row


def one_hot(row, count):
    lines = lax.broadcasted_iota(jnp.int32, (count, row.shape[1]), 0)
    return (lines == row).astype(jnp.float32)


def turning(rows, cols):
    count = rows * cols
    to = lax.broadcasted_iota(jnp.int32, (count, count), 0)
    at = lax.broadcasted_iota(jnp.int32, (count, count), 1)
    return ((at // cols == to % rows) & (at % cols == to // rows)).astype(jnp.float32).astype(jnp.bfloat16)


def repeat(count, unroll, step):
    if unroll:
        for n in range(count):
            step(n)
    else:
        lax.fori_loop(0, count, lambda n, _: step(n), None)


def pick_kernel(clu_ref, index_ref, raw_ref, out_ref, middle, *, second, unroll):
    clu = clu_ref[0]
    xs, occ, width = raw_ref.shape
    if second:
        parts = [
            one_hot(chosen(clu, [index_ref[c, pl.ds(s, 1), :] for s in range(index_ref.shape[1])]), occ).T
            for c in range(index_ref.shape[0])
        ]
        picks = jnp.concatenate(parts, axis=0)
    else:
        picks = one_hot(chosen(clu, [index_ref[pl.ds(c, 1), :] for c in range(index_ref.shape[0])]), occ).T
    picks = picks.astype(jnp.bfloat16)
    turn = turning(xs, GROUP)

    @functools.partial(repeat, xs, unroll)
    def _(x):
        middle[x] = jnp.dot(picks, raw_ref[x], preferred_element_type=jnp.float32).astype(jnp.bfloat16)

    @functools.partial(repeat, picks.shape[0] // GROUP, unroll)
    def _(g):
        lines = middle[:, pl.ds(g * GROUP, GROUP), :].reshape(xs * GROUP, width)
        out_ref[pl.ds(g * GROUP * xs, GROUP * xs), :] = jnp.dot(
            turn, lines, preferred_element_type=jnp.float32
        ).astype(jnp.bfloat16)


def pick(clu, index, raw, count, second, block, start, width):
    xs, occ, _ = raw.shape
    first = start // block
    return pl.pallas_call(
        functools.partial(pick_kernel, second=second, unroll=second),
        grid=(width // block,),
        in_specs=[
            pl.BlockSpec(memory_space=pltpu.SMEM),
            pl.BlockSpec(index.shape, lambda v: (0,) * index.ndim),
            pl.BlockSpec((xs, occ, block), lambda v: (0, 0, first + v)),
        ],
        out_specs=pl.BlockSpec((count * xs, block), lambda v: (0, v)),
        out_shape=jax.ShapeDtypeStruct((count * xs, width), jnp.bfloat16),
        scratch_shapes=[pltpu.VMEM((xs, count, block), jnp.bfloat16)],
        cost_estimate=pl.CostEstimate(
            flops=4 * xs * count * occ * width, bytes_accessed=2 * xs * (count + occ) * width, transcendentals=0
        ),
        name="pick_second" if second else "pick_owned",
    )(clu, index, raw)


def place_kernel(clu_ref, order_ref, back_ref, *rest, unroll):
    out_ref, middle = rest[-2:]
    clu = clu_ref[0]
    xs, occ, width = out_ref.shape
    spots = one_hot(
        chosen(clu, [order_ref[pl.ds(c, 1), :] for c in range(order_ref.shape[0])]), occ
    ).astype(jnp.bfloat16)
    turn = turning(GROUP, xs)

    @functools.partial(repeat, occ // GROUP, unroll)
    def _(g):
        lines = back_ref[pl.ds(g * GROUP * xs, GROUP * xs), :]
        middle[:, pl.ds(g * GROUP, GROUP), :] = (
            jnp.dot(turn, lines, preferred_element_type=jnp.float32)
            .astype(jnp.bfloat16)
            .reshape(xs, GROUP, width)
        )

    @functools.partial(repeat, xs, unroll)
    def _(x):
        out_ref[x] = jnp.dot(spots, middle[x], preferred_element_type=jnp.float32).astype(jnp.bfloat16)


def place(clu, order, back, placed, xs, virt, block, start):
    occ = order.shape[1]
    width = back.shape[1]
    first = start // block
    return pl.pallas_call(
        functools.partial(place_kernel, unroll=bool(placed)),
        grid=(width // block,),
        in_specs=[
            pl.BlockSpec(memory_space=pltpu.SMEM),
            pl.BlockSpec(order.shape, lambda v: (0, 0)),
            pl.BlockSpec((occ * xs, block), lambda v: (0, v)),
        ]
        + [pl.BlockSpec(memory_space=pl.ANY)] * len(placed),
        out_specs=pl.BlockSpec((xs, occ, block), lambda v: (0, 0, first + v)),
        out_shape=jax.ShapeDtypeStruct((xs, occ, virt), jnp.bfloat16),
        scratch_shapes=[pltpu.VMEM((xs, occ, block), jnp.bfloat16)],
        input_output_aliases={3: 0} if placed else {},
        cost_estimate=pl.CostEstimate(
            flops=4 * xs * occ * occ * width, bytes_accessed=4 * xs * occ * width, transcendentals=0
        ),
        name="place",
    )(clu, order, pltpu.with_memory_space_constraint(back, pltpu.HBM), *placed)


def gamma_kernel(
    slot_ref, first_ref, scale_ref, virt_row_ref, virt_col_ref, own_hbm, weight_hbm, fit_hbm, out_hbm,
    own, weight, fit, amplitude, total, rounded, blank, own_in, weight_in, fit_in, sent, blanked,
):
    slots = weight.shape[0]
    owned = out_hbm.shape[1]
    full, width = total.shape
    slot = [slot_ref[t] for t in range(slots)]
    first = [first_ref[t] for t in range(slots)]
    used = [functools.reduce(jnp.logical_or, [f == k for f in first]) for k in range(owned)]
    copy = pltpu.make_async_copy
    own_copy = [copy(own_hbm.at[:, first[t]], own.at[t], own_in.at[t]) for t in range(slots)]
    weight_copy = [copy(weight_hbm.at[slot[t]], weight.at[t], weight_in.at[t]) for t in range(slots)]
    fit_copy = [copy(fit_hbm.at[slot[t]], fit.at[t], fit_in.at[t]) for t in range(slots)]
    send = [copy(rounded.at[t], out_hbm.at[:, first[t]], sent.at[t]) for t in range(slots)]
    clear = [copy(blank, out_hbm.at[:, k], blanked.at[k]) for k in range(owned)]
    for t in range(slots):
        own_copy[t].start()
        weight_copy[t].start()
        fit_copy[t].start()
    blank[...] = jnp.zeros(blank.shape, blank.dtype)
    for k in range(owned):
        @pl.when(jnp.logical_not(used[k]))
        def _(k=k):
            clear[k].start()

    for t in range(slots):
        own_copy[t].wait()
        weight_copy[t].wait()
        crossed = jnp.dot(weight[t], own[t].reshape(full, width), preferred_element_type=jnp.float32)
        below = virt_col_ref[...] + virt_row_ref[...] - scale_ref[0, slot[t]] - scale_ref[1, slot[t]]
        amplitude[...] = (crossed * (scale_ref[2, slot[t]] / below)).astype(jnp.bfloat16)
        fit_copy[t].wait()
        part = jnp.dot(fit[t], amplitude[...], preferred_element_type=jnp.float32)
        if t > 0:
            part = part + jnp.where(first[t] == first[t - 1], total[...], 0.0)
        if t < slots - 1:
            total[...] = part
        rounded[t] = part.astype(jnp.bfloat16).reshape(rounded.shape[1:])
        if t < slots - 1:
            @pl.when(first[t] != first[t + 1])
            def _(t=t):
                send[t].start()
        else:
            send[t].start()

    for t in range(slots - 1):
        @pl.when(first[t] != first[t + 1])
        def _(t=t):
            send[t].wait()

    send[slots - 1].wait()
    for k in range(owned):
        @pl.when(jnp.logical_not(used[k]))
        def _(k=k):
            clear[k].wait()


def gamma_of(first, scale, own, weight, fit, virt_energy, start):
    sources, owned, xs, width = own.shape
    slots, virt, full = weight.shape
    number = jnp.arange(slots, dtype=jnp.int32)
    key = first * slots + number
    rank = jnp.sum((key[:, None] > key[None, :]).astype(jnp.int32), axis=1)
    at = (rank[None, :] == number[:, None]).astype(jnp.int32)
    hbm = pl.BlockSpec(memory_space=pltpu.HBM)
    smem = pl.BlockSpec(memory_space=pltpu.SMEM)
    vmem = pl.BlockSpec(memory_space=pltpu.VMEM)
    dma = pltpu.SemaphoreType.DMA
    return pl.pallas_call(
        gamma_kernel,
        in_specs=[smem, smem, smem, vmem, vmem, pl.BlockSpec(memory_space=pl.ANY), hbm, hbm],
        out_specs=hbm,
        out_shape=jax.ShapeDtypeStruct(own.shape, jnp.bfloat16),
        scratch_shapes=[
            pltpu.VMEM((slots, sources, xs, width), jnp.bfloat16),
            pltpu.VMEM((slots, virt, full), jnp.bfloat16),
            pltpu.VMEM((slots, full, virt), jnp.bfloat16),
            pltpu.VMEM((virt, width), jnp.bfloat16),
            pltpu.VMEM((full, width), jnp.float32),
            pltpu.VMEM((slots, sources, xs, width), jnp.bfloat16),
            pltpu.VMEM((sources, xs, width), jnp.bfloat16),
            dma((slots,)),
            dma((slots,)),
            dma((slots,)),
            dma((slots,)),
            dma((owned,)),
        ],
        cost_estimate=pl.CostEstimate(
            flops=4 * slots * full * virt * width, bytes_accessed=16 * full * virt * 2, transcendentals=0
        ),
        compiler_params=pltpu.CompilerParams(vmem_limit_bytes=52 * 1024 * 1024),
        name="gamma",
    )(
        jnp.sum(at * number[None, :], axis=1),
        jnp.sum(at * first[None, :], axis=1),
        scale,
        virt_energy[None, start : start + width],
        virt_energy[:, None],
        pltpu.with_memory_space_constraint(own, pltpu.HBM),
        pltpu.with_memory_space_constraint(weight, pltpu.HBM),
        pltpu.with_memory_space_constraint(fit, pltpu.HBM),
    )


def along_orb(block, dy, dz, dc):
    ny = lax.axis_size("orb") // (NZ * NC)
    pairs = [
        ((y * NZ + z) * NC + c, ((y + dy) % ny * NZ + (z + dz) % NZ) * NC + (c + dc) % NC)
        for y in range(ny)
        for z in range(NZ)
        for c in range(NC)
    ]
    return lax.ppermute(block, "orb", pairs)


def orb_place():
    here = lax.axis_index("orb")
    return here // (NZ * NC), here // NC % NZ, here % NC


def in_order(blocks):
    count = blocks.shape[0]
    ny = count // (NZ * NC)
    here_y, here_z, here_c = orb_place()
    number = jnp.arange(count, dtype=jnp.int32)
    y, z, c = number // (NZ * NC), number // NC % NZ, number % NC
    spot = ((here_c - c) % NC * ny + (here_y - y) % ny) * NZ + (here_z - z) % NZ
    return jnp.take(blocks, spot, axis=0, mode="clip")


def whole_metric(metric):
    orb_count = lax.axis_size("orb")
    ny = orb_count // (NZ * NC)
    block = metric.T
    q, p = block.shape
    got = [along_orb(block, 0, k, 0) for k in range(1, NZ)]
    column = jnp.stack([block] + got)
    got = [along_orb(column, k, 0, 0) for k in range(1, ny)]
    plane = jnp.stack([column] + got)
    got = [along_orb(plane, 0, 0, k) for k in range(1, NC)]
    every = jnp.stack([plane] + got).reshape(orb_count, q, p)
    return in_order(every).reshape(orb_count * q, p)


def exchange_staged(blocks):
    count, rows, lanes = blocks.shape
    ny = count // (NZ * NC)
    here_y, here_z, here_c = orb_place()
    number = jnp.arange(count, dtype=jnp.int32)
    k, y, c = number // (ny * NC), number // NC % ny, number % NC
    ready = jnp.take(blocks, (y * NZ + (here_z + k) % NZ) * NC + c, axis=0, mode="clip")
    ready = ready.reshape(NZ, ny * NC, rows, lanes)
    got = [along_orb(ready[n], 0, n, 0) for n in range(1, NZ)]
    held = jnp.stack([ready[0]] + got).reshape(count, rows, lanes)
    t, k, c = number // (NZ * NC), number // NC % NZ, number % NC
    ready = jnp.take(held, (k * ny + (here_y + t) % ny) * NC + c, axis=0, mode="clip")
    ready = ready.reshape(ny, NZ * NC, rows, lanes)
    got = [along_orb(ready[n], n, 0, 0) for n in range(1, ny)]
    held = jnp.stack([ready[0]] + got).reshape(count, rows, lanes)
    u, tk = number // (ny * NZ), number % (ny * NZ)
    ready = jnp.take(held, tk * NC + (here_c + u) % NC, axis=0, mode="clip")
    ready = ready.reshape(NC, ny * NZ, rows, lanes)
    got = [along_orb(ready[n], 0, 0, n) for n in range(1, NC)]
    return in_order(jnp.stack([ready[0]] + got).reshape(count, rows, lanes))


def window(
    integrals, metric, occ_energy, virt_energy, orbital_order, pair_first, pair_second, pair_live
):
    orb_count = lax.axis_size("orb")
    here_orb = lax.axis_index("orb")
    here_clu = lax.axis_index("clu")
    xs_rows, occ_count, virt = integrals.shape
    full_aux = metric.shape[0]
    owned = occ_count // orb_count
    slots = pair_second.shape[2]
    clu = here_clu.astype(jnp.int32)[None]

    wanted = pick(clu, pair_second.transpose(0, 2, 1), integrals, occ_count, True, BLOCK, 0, virt)
    seconds = lax.all_to_all(
        wanted.reshape(-1, xs_rows, virt), ("clu", "orb"), split_axis=0, concat_axis=0, tiled=True
    ).reshape(slots, full_aux, virt)

    block = virt // PARTS
    main = virt - block
    mine = pick(clu, orbital_order, integrals, occ_count, False, block, 0, main)
    rest = pick(clu, orbital_order, integrals, occ_count, False, block, main, block)
    own = lax.all_to_all(mine.reshape(orb_count, owned, xs_rows, main), "orb", split_axis=0, concat_axis=0, tiled=True)
    own_rest = exchange_staged(rest.reshape(orb_count, owned * xs_rows, block))
    own_rest = own_rest.reshape(orb_count, owned, xs_rows, block)

    turned = whole_metric(metric)
    fit = jnp.einsum("qp,spb->sqb", turned, seconds, preferred_element_type=jnp.float32).astype(jnp.bfloat16)
    weight = jnp.einsum("sqb,qp->sbp", fit, turned, preferred_element_type=jnp.float32).astype(jnp.bfloat16)

    first_slot = pair_first[0, 0]
    order = lax.dynamic_index_in_dim(orbital_order, here_clu, 0, keepdims=False)
    owned_orbs = lax.dynamic_slice_in_dim(order, here_orb * owned, owned) + here_clu * occ_count
    first_orb = jnp.take(owned_orbs, first_slot)
    own_second = lax.dynamic_slice(pair_second, (here_clu, here_orb, 0), (1, 1, slots))[0, 0]
    second_orb = own_second + jnp.arange(slots, dtype=jnp.int32) * occ_count
    scale = jnp.stack(
        [occ_energy[first_orb], occ_energy[second_orb], pair_live[0, 0].astype(jnp.float32)]
    )

    local = gamma_of(first_slot, scale, own, weight, fit, virt_energy, 0)
    back = lax.all_to_all(local, "orb", split_axis=0, concat_axis=0, tiled=True)
    local_rest = gamma_of(first_slot, scale, own_rest, weight, fit, virt_energy, main)
    back_rest = lax.all_to_all(local_rest, "orb", split_axis=0, concat_axis=0, tiled=True)
    lines = occ_count * xs_rows
    placed = place(clu, orbital_order, back.reshape(lines, main), (), xs_rows, virt, block, 0)
    return place(clu, orbital_order, back_rest.reshape(lines, block), (placed,), xs_rows, virt, block, main)


def solution(mesh):
    in_specs = (
        P("orb", "clu", None),
        P(None, "orb"),
        P(),
        P(),
        P(),
        P("clu", "orb", None),
        P(),
        P("clu", "orb", None),
    )
    out_specs = P("orb", "clu", None)
    return jax.shard_map(window, mesh=mesh, in_specs=in_specs, out_specs=out_specs, check_vma=False)
```

```python
import functools

import jax
import jax.numpy as jnp
from jax import lax
from jax.experimental import pallas as pl
from jax.experimental.pallas import tpu as pltpu
from jax.sharding import PartitionSpec as P


BLOCK, GROUP = 256, 16
PARTS = 4
NZ, NC = 8, 2


def chosen(clu, rows):
    row = rows[0]
    for i in range(1, len(rows)):
        row = jnp.where(clu == i, rows[i], row)
    return row


def one_hot(row, count):
    lines = lax.broadcasted_iota(jnp.int32, (count, row.shape[1]), 0)
    return (lines == row).astype(jnp.float32)


def turning(rows, cols):
    count = rows * cols
    to = lax.broadcasted_iota(jnp.int32, (count, count), 0)
    at = lax.broadcasted_iota(jnp.int32, (count, count), 1)
    return ((at // cols == to % rows) & (at % cols == to // rows)).astype(jnp.float32).astype(jnp.bfloat16)


def repeat(count, unroll, step):
    if unroll:
        for n in range(count):
            step(n)
    else:
        lax.fori_loop(0, count, lambda n, _: step(n), None)


def pick_kernel(clu_ref, index_ref, raw_ref, out_ref, middle, *, second, unroll):
    clu = clu_ref[0]
    xs, occ, width = raw_ref.shape
    if second:
        parts = [
            one_hot(chosen(clu, [index_ref[c, pl.ds(s, 1), :] for s in range(index_ref.shape[1])]), occ).T
            for c in range(index_ref.shape[0])
        ]
        picks = jnp.concatenate(parts, axis=0)
    else:
        picks = one_hot(chosen(clu, [index_ref[pl.ds(c, 1), :] for c in range(index_ref.shape[0])]), occ).T
    picks = picks.astype(jnp.bfloat16)
    turn = turning(xs, GROUP)

    @functools.partial(repeat, xs, unroll)
    def _(x):
        middle[x] = jnp.dot(picks, raw_ref[x], preferred_element_type=jnp.float32).astype(jnp.bfloat16)

    @functools.partial(repeat, picks.shape[0] // GROUP, unroll)
    def _(g):
        lines = middle[:, pl.ds(g * GROUP, GROUP), :].reshape(xs * GROUP, width)
        out_ref[pl.ds(g * GROUP * xs, GROUP * xs), :] = jnp.dot(
            turn, lines, preferred_element_type=jnp.float32
        ).astype(jnp.bfloat16)


def pick(clu, index, raw, count, second, block, start, width):
    xs, occ, _ = raw.shape
    first = start // block
    return pl.pallas_call(
        functools.partial(pick_kernel, second=second, unroll=second),
        grid=(width // block,),
        in_specs=[
            pl.BlockSpec(memory_space=pltpu.SMEM),
            pl.BlockSpec(index.shape, lambda v: (0,) * index.ndim),
            pl.BlockSpec((xs, occ, block), lambda v: (0, 0, first + v)),
        ],
        out_specs=pl.BlockSpec((count * xs, block), lambda v: (0, v)),
        out_shape=jax.ShapeDtypeStruct((count * xs, width), jnp.bfloat16),
        scratch_shapes=[pltpu.VMEM((xs, count, block), jnp.bfloat16)],
        cost_estimate=pl.CostEstimate(
            flops=4 * xs * count * occ * width, bytes_accessed=2 * xs * (count + occ) * width, transcendentals=0
        ),
        name="pick_second" if second else "pick_owned",
    )(clu, index, raw)


def place_kernel(clu_ref, order_ref, back_ref, out_ref, middle):
    clu = clu_ref[0]
    xs, occ, width = out_ref.shape
    spots = one_hot(
        chosen(clu, [order_ref[pl.ds(c, 1), :] for c in range(order_ref.shape[0])]), occ
    ).astype(jnp.bfloat16)
    turn = turning(GROUP, xs)
    for g in range(occ // GROUP):
        lines = back_ref[g * GROUP * xs : (g + 1) * GROUP * xs, :]
        middle[:, g * GROUP : (g + 1) * GROUP, :] = (
            jnp.dot(turn, lines, preferred_element_type=jnp.float32)
            .astype(jnp.bfloat16)
            .reshape(xs, GROUP, width)
        )
    for x in range(xs):
        out_ref[x] = jnp.dot(spots, middle[x], preferred_element_type=jnp.float32).astype(jnp.bfloat16)


def place(clu, order, back, xs):
    occ = order.shape[1]
    virt = back.shape[1]
    return pl.pallas_call(
        place_kernel,
        grid=(virt // BLOCK,),
        in_specs=[
            pl.BlockSpec(memory_space=pltpu.SMEM),
            pl.BlockSpec(order.shape, lambda v: (0, 0)),
            pl.BlockSpec((occ * xs, BLOCK), lambda v: (0, v)),
        ],
        out_specs=pl.BlockSpec((xs, occ, BLOCK), lambda v: (0, 0, v)),
        out_shape=jax.ShapeDtypeStruct((xs, occ, virt), jnp.bfloat16),
        scratch_shapes=[pltpu.VMEM((xs, occ, BLOCK), jnp.bfloat16)],
        cost_estimate=pl.CostEstimate(
            flops=4 * xs * occ * occ * virt, bytes_accessed=4 * xs * occ * virt, transcendentals=0
        ),
        name="place",
    )(clu, order, back)


def gamma_kernel(
    slot_ref, first_ref, scale_ref, virt_row_ref, virt_col_ref, main_hbm, rest_hbm, weight_hbm, fit_hbm, out_hbm,
    own, weight, fit, amplitude, total, rounded, blank, main_in, rest_in, weight_in, fit_in, sent, blanked,
):
    slots = weight.shape[0]
    owned = out_hbm.shape[1]
    full, width = total.shape
    slot = [slot_ref[t] for t in range(slots)]
    first = [first_ref[t] for t in range(slots)]
    used = [functools.reduce(jnp.logical_or, [f == k for f in first]) for k in range(owned)]
    copy = pltpu.make_async_copy
    main = main_hbm.shape[3]
    main_copy = [
        copy(main_hbm.at[:, first[t]], own.at[t, :, :, pl.ds(0, main)], main_in.at[t]) for t in range(slots)
    ]
    rest_copy = [
        copy(rest_hbm.at[:, first[t]], own.at[t, :, :, pl.ds(main, width - main)], rest_in.at[t])
        for t in range(slots)
    ]
    weight_copy = [copy(weight_hbm.at[slot[t]], weight.at[t], weight_in.at[t]) for t in range(slots)]
    fit_copy = [copy(fit_hbm.at[slot[t]], fit.at[t], fit_in.at[t]) for t in range(slots)]
    send = [copy(rounded.at[t], out_hbm.at[:, first[t]], sent.at[t]) for t in range(slots)]
    clear = [copy(blank, out_hbm.at[:, k], blanked.at[k]) for k in range(owned)]
    for t in range(slots):
        main_copy[t].start()
        rest_copy[t].start()
        weight_copy[t].start()
        fit_copy[t].start()
    blank[...] = jnp.zeros(blank.shape, blank.dtype)
    for k in range(owned):
        @pl.when(jnp.logical_not(used[k]))
        def _(k=k):
            clear[k].start()

    for t in range(slots):
        main_copy[t].wait()
        rest_copy[t].wait()
        weight_copy[t].wait()
        crossed = jnp.dot(weight[t], own[t].reshape(full, width), preferred_element_type=jnp.float32)
        below = virt_col_ref[...] + virt_row_ref[...] - scale_ref[0, slot[t]] - scale_ref[1, slot[t]]
        amplitude[...] = (crossed * (scale_ref[2, slot[t]] / below)).astype(jnp.bfloat16)
        fit_copy[t].wait()
        part = jnp.dot(fit[t], amplitude[...], preferred_element_type=jnp.float32)
        if t > 0:
            part = part + jnp.where(first[t] == first[t - 1], total[...], 0.0)
        if t < slots - 1:
            total[...] = part
        rounded[t] = part.astype(jnp.bfloat16).reshape(rounded.shape[1:])
        if t < slots - 1:
            @pl.when(first[t] != first[t + 1])
            def _(t=t):
                send[t].start()
        else:
            send[t].start()

    for t in range(slots - 1):
        @pl.when(first[t] != first[t + 1])
        def _(t=t):
            send[t].wait()

    send[slots - 1].wait()
    for k in range(owned):
        @pl.when(jnp.logical_not(used[k]))
        def _(k=k):
            clear[k].wait()


def gamma_of(first, scale, main, rest, weight, fit, virt_energy):
    sources, owned, xs, _ = main.shape
    slots, virt, full = weight.shape
    width = virt
    number = jnp.arange(slots, dtype=jnp.int32)
    key = first * slots + number
    rank = jnp.sum((key[:, None] > key[None, :]).astype(jnp.int32), axis=1)
    at = (rank[None, :] == number[:, None]).astype(jnp.int32)
    hbm = pl.BlockSpec(memory_space=pltpu.HBM)
    anywhere = pl.BlockSpec(memory_space=pl.ANY)
    smem = pl.BlockSpec(memory_space=pltpu.SMEM)
    vmem = pl.BlockSpec(memory_space=pltpu.VMEM)
    dma = pltpu.SemaphoreType.DMA
    return pl.pallas_call(
        gamma_kernel,
        in_specs=[smem, smem, smem, vmem, vmem, anywhere, anywhere, hbm, hbm],
        out_specs=hbm,
        out_shape=jax.ShapeDtypeStruct((sources, owned, xs, virt), jnp.bfloat16),
        scratch_shapes=[
            pltpu.VMEM((slots, sources, xs, width), jnp.bfloat16),
            pltpu.VMEM((slots, virt, full), jnp.bfloat16),
            pltpu.VMEM((slots, full, virt), jnp.bfloat16),
            pltpu.VMEM((virt, width), jnp.bfloat16),
            pltpu.VMEM((full, width), jnp.float32),
            pltpu.VMEM((slots, sources, xs, width), jnp.bfloat16),
            pltpu.VMEM((sources, xs, width), jnp.bfloat16),
            dma((slots,)),
            dma((slots,)),
            dma((slots,)),
            dma((slots,)),
            dma((slots,)),
            dma((owned,)),
        ],
        cost_estimate=pl.CostEstimate(
            flops=4 * slots * full * virt * width, bytes_accessed=16 * full * virt * 2, transcendentals=0
        ),
        compiler_params=pltpu.CompilerParams(vmem_limit_bytes=28 * 1024 * 1024),
        name="gamma",
    )(
        jnp.sum(at * number[None, :], axis=1),
        jnp.sum(at * first[None, :], axis=1),
        scale,
        virt_energy[None, :],
        virt_energy[:, None],
        main,
        pltpu.with_memory_space_constraint(rest, pltpu.HBM),
        pltpu.with_memory_space_constraint(weight, pltpu.HBM),
        pltpu.with_memory_space_constraint(fit, pltpu.HBM),
    )


def along_orb(block, dy, dz, dc):
    ny = lax.axis_size("orb") // (NZ * NC)
    pairs = [
        ((y * NZ + z) * NC + c, ((y + dy) % ny * NZ + (z + dz) % NZ) * NC + (c + dc) % NC)
        for y in range(ny)
        for z in range(NZ)
        for c in range(NC)
    ]
    return lax.ppermute(block, "orb", pairs)


def orb_place():
    here = lax.axis_index("orb")
    return here // (NZ * NC), here // NC % NZ, here % NC


def in_order(blocks):
    count = blocks.shape[0]
    ny = count // (NZ * NC)
    here_y, here_z, here_c = orb_place()
    number = jnp.arange(count, dtype=jnp.int32)
    y, z, c = number // (NZ * NC), number // NC % NZ, number % NC
    spot = ((here_c - c) % NC * ny + (here_y - y) % ny) * NZ + (here_z - z) % NZ
    return jnp.take(blocks, spot, axis=0, mode="clip")


def whole_metric(metric):
    orb_count = lax.axis_size("orb")
    ny = orb_count // (NZ * NC)
    block = metric.T
    q, p = block.shape
    got = [along_orb(block, 0, k, 0) for k in range(1, NZ)]
    column = jnp.stack([block] + got)
    got = [along_orb(column, k, 0, 0) for k in range(1, ny)]
    plane = jnp.stack([column] + got)
    got = [along_orb(plane, 0, 0, k) for k in range(1, NC)]
    every = jnp.stack([plane] + got).reshape(orb_count, q, p)
    return in_order(every).reshape(orb_count * q, p)


def exchange_staged(blocks):
    count, rows, lanes = blocks.shape
    ny = count // (NZ * NC)
    here_y, here_z, here_c = orb_place()
    number = jnp.arange(count, dtype=jnp.int32)
    k, y, c = number // (ny * NC), number // NC % ny, number % NC
    ready = jnp.take(blocks, (y * NZ + (here_z + k) % NZ) * NC + c, axis=0, mode="clip")
    ready = ready.reshape(NZ, ny * NC, rows, lanes)
    got = [along_orb(ready[n], 0, n, 0) for n in range(1, NZ)]
    held = jnp.stack([ready[0]] + got).reshape(count, rows, lanes)
    t, k, c = number // (NZ * NC), number // NC % NZ, number % NC
    ready = jnp.take(held, (k * ny + (here_y + t) % ny) * NC + c, axis=0, mode="clip")
    ready = ready.reshape(ny, NZ * NC, rows, lanes)
    got = [along_orb(ready[n], n, 0, 0) for n in range(1, ny)]
    held = jnp.stack([ready[0]] + got).reshape(count, rows, lanes)
    u, tk = number // (ny * NZ), number % (ny * NZ)
    ready = jnp.take(held, tk * NC + (here_c + u) % NC, axis=0, mode="clip")
    ready = ready.reshape(NC, ny * NZ, rows, lanes)
    got = [along_orb(ready[n], 0, 0, n) for n in range(1, NC)]
    return in_order(jnp.stack([ready[0]] + got).reshape(count, rows, lanes))


def window(
    integrals, metric, occ_energy, virt_energy, orbital_order, pair_first, pair_second, pair_live
):
    orb_count = lax.axis_size("orb")
    here_orb = lax.axis_index("orb")
    here_clu = lax.axis_index("clu")
    xs_rows, occ_count, virt = integrals.shape
    full_aux = metric.shape[0]
    owned = occ_count // orb_count
    slots = pair_second.shape[2]
    clu = here_clu.astype(jnp.int32)[None]

    wanted = pick(clu, pair_second.transpose(0, 2, 1), integrals, occ_count, True, BLOCK, 0, virt)
    seconds = lax.all_to_all(
        wanted.reshape(-1, xs_rows, virt), ("clu", "orb"), split_axis=0, concat_axis=0, tiled=True
    ).reshape(slots, full_aux, virt)

    block = virt // PARTS
    main = virt - block
    mine = pick(clu, orbital_order, integrals, occ_count, False, block, 0, main)
    rest = pick(clu, orbital_order, integrals, occ_count, False, block, main, block)
    own = lax.all_to_all(mine.reshape(orb_count, owned, xs_rows, main), "orb", split_axis=0, concat_axis=0, tiled=True)
    own_rest = exchange_staged(rest.reshape(orb_count, owned * xs_rows, block))
    own_rest = own_rest.reshape(orb_count, owned, xs_rows, block)

    turned = whole_metric(metric)
    fit = jnp.einsum("qp,spb->sqb", turned, seconds, preferred_element_type=jnp.float32).astype(jnp.bfloat16)
    weight = jnp.einsum("sqb,qp->sbp", fit, turned, preferred_element_type=jnp.float32).astype(jnp.bfloat16)

    first_slot = pair_first[0, 0]
    order = lax.dynamic_index_in_dim(orbital_order, here_clu, 0, keepdims=False)
    owned_orbs = lax.dynamic_slice_in_dim(order, here_orb * owned, owned) + here_clu * occ_count
    first_orb = jnp.take(owned_orbs, first_slot)
    own_second = lax.dynamic_slice(pair_second, (here_clu, here_orb, 0), (1, 1, slots))[0, 0]
    second_orb = own_second + jnp.arange(slots, dtype=jnp.int32) * occ_count
    scale = jnp.stack(
        [occ_energy[first_orb], occ_energy[second_orb], pair_live[0, 0].astype(jnp.float32)]
    )

    local = gamma_of(first_slot, scale, own, own_rest, weight, fit, virt_energy)
    back = lax.all_to_all(local, "orb", split_axis=0, concat_axis=0, tiled=True)
    return place(clu, orbital_order, back.reshape(occ_count * xs_rows, virt), xs_rows)


def solution(mesh):
    in_specs = (
        P("orb", "clu", None),
        P(None, "orb"),
        P(),
        P(),
        P(),
        P("clu", "orb", None),
        P(),
        P("clu", "orb", None),
    )
    out_specs = P("orb", "clu", None)
    return jax.shard_map(window, mesh=mesh, in_specs=in_specs, out_specs=out_specs, check_vma=False)
```

```python
import functools

import jax
import jax.numpy as jnp
from jax import lax
from jax.experimental import pallas as pl
from jax.experimental.pallas import tpu as pltpu
from jax.sharding import PartitionSpec as P


BLOCK, GROUP = 256, 16
PARTS = 4
NZ, NC = 8, 2


def chosen(clu, rows):
    row = rows[0]
    for i in range(1, len(rows)):
        row = jnp.where(clu == i, rows[i], row)
    return row


def one_hot(row, count):
    lines = lax.broadcasted_iota(jnp.int32, (count, row.shape[1]), 0)
    return (lines == row).astype(jnp.float32)


def turning(rows, cols):
    count = rows * cols
    to = lax.broadcasted_iota(jnp.int32, (count, count), 0)
    at = lax.broadcasted_iota(jnp.int32, (count, count), 1)
    return ((at // cols == to % rows) & (at % cols == to // rows)).astype(jnp.float32).astype(jnp.bfloat16)


def repeat(count, unroll, step):
    if unroll:
        for n in range(count):
            step(n)
    else:
        lax.fori_loop(0, count, lambda n, _: step(n), None)


def pick_kernel(clu_ref, index_ref, raw_ref, out_ref, middle, *, second, unroll):
    clu = clu_ref[0]
    xs, occ, width = raw_ref.shape
    if second:
        parts = [
            one_hot(chosen(clu, [index_ref[c, pl.ds(s, 1), :] for s in range(index_ref.shape[1])]), occ).T
            for c in range(index_ref.shape[0])
        ]
        picks = jnp.concatenate(parts, axis=0)
    else:
        picks = one_hot(chosen(clu, [index_ref[pl.ds(c, 1), :] for c in range(index_ref.shape[0])]), occ).T
    picks = picks.astype(jnp.bfloat16)
    turn = turning(xs, GROUP)

    @functools.partial(repeat, xs, unroll)
    def _(x):
        middle[x] = jnp.dot(picks, raw_ref[x], preferred_element_type=jnp.float32).astype(jnp.bfloat16)

    @functools.partial(repeat, picks.shape[0] // GROUP, unroll)
    def _(g):
        lines = middle[:, pl.ds(g * GROUP, GROUP), :].reshape(xs * GROUP, width)
        out_ref[pl.ds(g * GROUP * xs, GROUP * xs), :] = jnp.dot(
            turn, lines, preferred_element_type=jnp.float32
        ).astype(jnp.bfloat16)


def pick(clu, index, raw, count, second, block, start, width):
    xs, occ, _ = raw.shape
    first = start // block
    return pl.pallas_call(
        functools.partial(pick_kernel, second=second, unroll=second),
        grid=(width // block,),
        in_specs=[
            pl.BlockSpec(memory_space=pltpu.SMEM),
            pl.BlockSpec(index.shape, lambda v: (0,) * index.ndim),
            pl.BlockSpec((xs, occ, block), lambda v: (0, 0, first + v)),
        ],
        out_specs=pl.BlockSpec((count * xs, block), lambda v: (0, v)),
        out_shape=jax.ShapeDtypeStruct((count * xs, width), jnp.bfloat16),
        scratch_shapes=[pltpu.VMEM((xs, count, block), jnp.bfloat16)],
        cost_estimate=pl.CostEstimate(
            flops=4 * xs * count * occ * width, bytes_accessed=2 * xs * (count + occ) * width, transcendentals=0
        ),
        name="pick_second" if second else "pick_owned",
    )(clu, index, raw)


def place_kernel(clu_ref, order_ref, back_ref, out_ref, middle):
    clu = clu_ref[0]
    xs, occ, width = out_ref.shape
    spots = one_hot(
        chosen(clu, [order_ref[pl.ds(c, 1), :] for c in range(order_ref.shape[0])]), occ
    ).astype(jnp.bfloat16)
    turn = turning(GROUP, xs)
    for g in range(occ // GROUP):
        lines = back_ref[g * GROUP * xs : (g + 1) * GROUP * xs, :]
        middle[:, g * GROUP : (g + 1) * GROUP, :] = (
            jnp.dot(turn, lines, preferred_element_type=jnp.float32)
            .astype(jnp.bfloat16)
            .reshape(xs, GROUP, width)
        )
    for x in range(xs):
        out_ref[x] = jnp.dot(spots, middle[x], preferred_element_type=jnp.float32).astype(jnp.bfloat16)


def place(clu, order, back, xs):
    occ = order.shape[1]
    virt = back.shape[1]
    return pl.pallas_call(
        place_kernel,
        grid=(virt // BLOCK,),
        in_specs=[
            pl.BlockSpec(memory_space=pltpu.SMEM),
            pl.BlockSpec(order.shape, lambda v: (0, 0)),
            pl.BlockSpec((occ * xs, BLOCK), lambda v: (0, v)),
        ],
        out_specs=pl.BlockSpec((xs, occ, BLOCK), lambda v: (0, 0, v)),
        out_shape=jax.ShapeDtypeStruct((xs, occ, virt), jnp.bfloat16),
        scratch_shapes=[pltpu.VMEM((xs, occ, BLOCK), jnp.bfloat16)],
        cost_estimate=pl.CostEstimate(
            flops=4 * xs * occ * occ * virt, bytes_accessed=4 * xs * occ * virt, transcendentals=0
        ),
        name="place",
    )(clu, order, back)


def gamma_kernel(
    slot_ref, first_ref, scale_ref, virt_row_ref, virt_col_ref, main_hbm, rest_hbm, weight_hbm, fit_hbm, out_hbm,
    own, weight, fit, amplitude, total, rounded, blank, main_in, rest_in, weight_in, fit_in, sent, blanked,
):
    slots = weight.shape[0]
    owned = out_hbm.shape[1]
    full, width = total.shape
    slot = [slot_ref[t] for t in range(slots)]
    first = [first_ref[t] for t in range(slots)]
    used = [functools.reduce(jnp.logical_or, [f == k for f in first]) for k in range(owned)]
    copy = pltpu.make_async_copy
    main = main_hbm.shape[3]
    main_copy = [
        copy(main_hbm.at[:, first[t]], own.at[t, :, :, pl.ds(0, main)], main_in.at[t]) for t in range(slots)
    ]
    rest_copy = [
        copy(rest_hbm.at[:, first[t]], own.at[t, :, :, pl.ds(main, width - main)], rest_in.at[t])
        for t in range(slots)
    ]
    weight_copy = [copy(weight_hbm.at[slot[t]], weight.at[t], weight_in.at[t]) for t in range(slots)]
    fit_copy = [copy(fit_hbm.at[slot[t]], fit.at[t], fit_in.at[t]) for t in range(slots)]
    send = [copy(rounded.at[t], out_hbm.at[:, first[t]], sent.at[t]) for t in range(slots)]
    clear = [copy(blank, out_hbm.at[:, k], blanked.at[k]) for k in range(owned)]
    for t in range(slots):
        main_copy[t].start()
        rest_copy[t].start()
        weight_copy[t].start()
        fit_copy[t].start()
    blank[...] = jnp.zeros(blank.shape, blank.dtype)
    for k in range(owned):
        @pl.when(jnp.logical_not(used[k]))
        def _(k=k):
            clear[k].start()

    for t in range(slots):
        main_copy[t].wait()
        rest_copy[t].wait()
        weight_copy[t].wait()
        crossed = jnp.dot(weight[t], own[t].reshape(full, width), preferred_element_type=jnp.float32)
        below = virt_col_ref[...] + virt_row_ref[...] - scale_ref[0, slot[t]] - scale_ref[1, slot[t]]
        amplitude[...] = (crossed * (scale_ref[2, slot[t]] / below)).astype(jnp.bfloat16)
        fit_copy[t].wait()
        part = jnp.dot(fit[t], amplitude[...], preferred_element_type=jnp.float32)
        if t > 0:
            part = part + jnp.where(first[t] == first[t - 1], total[...], 0.0)
        if t < slots - 1:
            total[...] = part
        rounded[t] = part.astype(jnp.bfloat16).reshape(rounded.shape[1:])
        if t < slots - 1:
            @pl.when(first[t] != first[t + 1])
            def _(t=t):
                send[t].start()
        else:
            send[t].start()

    for t in range(slots - 1):
        @pl.when(first[t] != first[t + 1])
        def _(t=t):
            send[t].wait()

    send[slots - 1].wait()
    for k in range(owned):
        @pl.when(jnp.logical_not(used[k]))
        def _(k=k):
            clear[k].wait()


def gamma_of(first, scale, main, rest, weight, fit, virt_energy):
    sources, owned, xs, _ = main.shape
    slots, virt, full = weight.shape
    width = virt
    number = jnp.arange(slots, dtype=jnp.int32)
    key = first * slots + number
    rank = jnp.sum((key[:, None] > key[None, :]).astype(jnp.int32), axis=1)
    at = (rank[None, :] == number[:, None]).astype(jnp.int32)
    hbm = pl.BlockSpec(memory_space=pltpu.HBM)
    anywhere = pl.BlockSpec(memory_space=pl.ANY)
    smem = pl.BlockSpec(memory_space=pltpu.SMEM)
    vmem = pl.BlockSpec(memory_space=pltpu.VMEM)
    dma = pltpu.SemaphoreType.DMA
    return pl.pallas_call(
        gamma_kernel,
        in_specs=[smem, smem, smem, vmem, vmem, anywhere, anywhere, hbm, hbm],
        out_specs=hbm,
        out_shape=jax.ShapeDtypeStruct((sources, owned, xs, virt), jnp.bfloat16),
        scratch_shapes=[
            pltpu.VMEM((slots, sources, xs, width), jnp.bfloat16),
            pltpu.VMEM((slots, virt, full), jnp.bfloat16),
            pltpu.VMEM((slots, full, virt), jnp.bfloat16),
            pltpu.VMEM((virt, width), jnp.bfloat16),
            pltpu.VMEM((full, width), jnp.float32),
            pltpu.VMEM((slots, sources, xs, width), jnp.bfloat16),
            pltpu.VMEM((sources, xs, width), jnp.bfloat16),
            dma((slots,)),
            dma((slots,)),
            dma((slots,)),
            dma((slots,)),
            dma((slots,)),
            dma((owned,)),
        ],
        cost_estimate=pl.CostEstimate(
            flops=4 * slots * full * virt * width, bytes_accessed=16 * full * virt * 2, transcendentals=0
        ),
        compiler_params=pltpu.CompilerParams(vmem_limit_bytes=28 * 1024 * 1024),
        name="gamma",
    )(
        jnp.sum(at * number[None, :], axis=1),
        jnp.sum(at * first[None, :], axis=1),
        scale,
        virt_energy[None, :],
        virt_energy[:, None],
        main,
        pltpu.with_memory_space_constraint(rest, pltpu.HBM),
        pltpu.with_memory_space_constraint(weight, pltpu.HBM),
        pltpu.with_memory_space_constraint(fit, pltpu.HBM),
    )


def along_orb(block, dy, dz, dc):
    ny = lax.axis_size("orb") // (NZ * NC)
    pairs = [
        ((y * NZ + z) * NC + c, ((y + dy) % ny * NZ + (z + dz) % NZ) * NC + (c + dc) % NC)
        for y in range(ny)
        for z in range(NZ)
        for c in range(NC)
    ]
    return lax.ppermute(block, "orb", pairs)


def orb_place():
    here = lax.axis_index("orb")
    return here // (NZ * NC), here // NC % NZ, here % NC


def in_order(blocks):
    count = blocks.shape[0]
    ny = count // (NZ * NC)
    here_y, here_z, here_c = orb_place()
    number = jnp.arange(count, dtype=jnp.int32)
    y, z, c = number // (NZ * NC), number // NC % NZ, number % NC
    spot = ((here_c - c) % NC * ny + (here_y - y) % ny) * NZ + (here_z - z) % NZ
    return jnp.take(blocks, spot, axis=0, mode="clip")


def whole_metric(metric):
    orb_count = lax.axis_size("orb")
    ny = orb_count // (NZ * NC)
    block = metric.T
    q, p = block.shape
    got = [along_orb(block, 0, k, 0) for k in range(1, NZ)]
    column = jnp.stack([block] + got)
    got = [along_orb(column, k, 0, 0) for k in range(1, ny)]
    plane = jnp.stack([column] + got)
    got = [along_orb(plane, 0, 0, k) for k in range(1, NC)]
    every = jnp.stack([plane] + got).reshape(orb_count, q, p)
    return in_order(every).reshape(orb_count * q, p)


def exchange_staged(blocks):
    count, rows, lanes = blocks.shape
    ny = count // (NZ * NC)
    here_y, here_z, here_c = orb_place()
    number = jnp.arange(count, dtype=jnp.int32)
    u, yz = number // (ny * NZ), number % (ny * NZ)
    ready = jnp.take(blocks, yz * NC + (here_c + u) % NC, axis=0, mode="clip")
    ready = ready.reshape(NC, ny * NZ, rows, lanes)
    got = [along_orb(ready[n], 0, 0, n) for n in range(1, NC)]
    held = jnp.stack([ready[0]] + got).reshape(count, rows, lanes)
    t, u, z = number // (NC * NZ), number // NZ % NC, number % NZ
    ready = jnp.take(held, (u * ny + (here_y + t) % ny) * NZ + z, axis=0, mode="clip")
    ready = ready.reshape(ny, NC * NZ, rows, lanes)
    got = [along_orb(ready[n], n, 0, 0) for n in range(1, ny)]
    held = jnp.stack([ready[0]] + got).reshape(count, rows, lanes)
    k, tu = number // (ny * NC), number % (ny * NC)
    ready = jnp.take(held, tu * NZ + (here_z + k) % NZ, axis=0, mode="clip")
    ready = ready.reshape(NZ, ny * NC, rows, lanes)
    got = [along_orb(ready[n], 0, n, 0) for n in range(1, NZ)]
    held = jnp.stack([ready[0]] + got).reshape(count, rows, lanes)
    y, z, c = number // (NZ * NC), number // NC % NZ, number % NC
    spot = ((here_z - z) % NZ * ny + (here_y - y) % ny) * NC + (here_c - c) % NC
    return jnp.take(held, spot, axis=0, mode="clip")


def window(
    integrals, metric, occ_energy, virt_energy, orbital_order, pair_first, pair_second, pair_live
):
    orb_count = lax.axis_size("orb")
    here_orb = lax.axis_index("orb")
    here_clu = lax.axis_index("clu")
    xs_rows, occ_count, virt = integrals.shape
    full_aux = metric.shape[0]
    owned = occ_count // orb_count
    slots = pair_second.shape[2]
    clu = here_clu.astype(jnp.int32)[None]

    wanted = pick(clu, pair_second.transpose(0, 2, 1), integrals, occ_count, True, BLOCK, 0, virt)
    seconds = lax.all_to_all(
        wanted.reshape(-1, xs_rows, virt), ("clu", "orb"), split_axis=0, concat_axis=0, tiled=True
    ).reshape(slots, full_aux, virt)

    block = virt // PARTS
    main = virt - block
    mine = pick(clu, orbital_order, integrals, occ_count, False, block, 0, main)
    rest = pick(clu, orbital_order, integrals, occ_count, False, block, main, block)
    own = lax.all_to_all(mine.reshape(orb_count, owned, xs_rows, main), "orb", split_axis=0, concat_axis=0, tiled=True)
    own_rest = exchange_staged(rest.reshape(orb_count, owned * xs_rows, block))
    own_rest = own_rest.reshape(orb_count, owned, xs_rows, block)

    turned = whole_metric(metric)
    fit = jnp.einsum("qp,spb->sqb", turned, seconds, preferred_element_type=jnp.float32).astype(jnp.bfloat16)
    weight = jnp.einsum("sqb,qp->sbp", fit, turned, preferred_element_type=jnp.float32).astype(jnp.bfloat16)

    first_slot = pair_first[0, 0]
    order = lax.dynamic_index_in_dim(orbital_order, here_clu, 0, keepdims=False)
    owned_orbs = lax.dynamic_slice_in_dim(order, here_orb * owned, owned) + here_clu * occ_count
    first_orb = jnp.take(owned_orbs, first_slot)
    own_second = lax.dynamic_slice(pair_second, (here_clu, here_orb, 0), (1, 1, slots))[0, 0]
    second_orb = own_second + jnp.arange(slots, dtype=jnp.int32) * occ_count
    scale = jnp.stack(
        [occ_energy[first_orb], occ_energy[second_orb], pair_live[0, 0].astype(jnp.float32)]
    )

    local = gamma_of(first_slot, scale, own, own_rest, weight, fit, virt_energy)
    back = lax.all_to_all(local, "orb", split_axis=0, concat_axis=0, tiled=True)
    return place(clu, orbital_order, back.reshape(occ_count * xs_rows, virt), xs_rows)


def solution(mesh):
    in_specs = (
        P("orb", "clu", None),
        P(None, "orb"),
        P(),
        P(),
        P(),
        P("clu", "orb", None),
        P(),
        P("clu", "orb", None),
    )
    out_specs = P("orb", "clu", None)
    return jax.shard_map(window, mesh=mesh, in_specs=in_specs, out_specs=out_specs, check_vma=False)
```
